32 devices in a mesh: image: 4 (over y, x), space: 8 (over z, core).
Axes of the slice: x: 2, y: 2, z: 4, core: 2. Of those that a mesh axis runs over, the one named last changes fastest.
Arguments:
- positions: float32 [4, 3, 8192], P('image', None, 'space'), may hold values from -20 to 20
- neighbours: int32 [64, 3], replicated, may hold values from 0 to 4
- brackets: int32 [4], P('image'), may hold values from 0 to 2, as said below
- codes: int32 [4], P('image'), may hold values from 0 to 65535
Outputs:
- new_images: float32 [4, 3, 8192], P('image', None, 'space')
- arc_fraction: float32 [4], P('image')
The draws below stay inside these ranges and needn't reach their ends.
Inputs may be any that keep to these rules, and one draw needn't show every extreme that they name: brackets[j] lies between j - 1 and j + 1 - 1; both ends of that window are reached.
All inputs are finite; a program needn't handle non-finite values.
Results may differ from the reference program's by a relative error of at most 0.0003.
Values sent between devices are 32-bit elements; how exact they have to be, the bound alone decides.
No kernel may reach another device: no remote copies, remote signals or barrier semaphores. Data moves between devices by JAX's collectives and lax.ppermute only.
A program may use at most 64 MiB of HBM per device.

```python
import jax
import jax.numpy as jnp
from jax import lax

IMG_DEV = 1
BEADS_DEV = 1024
PROT_DEV = 128
BLOCK = 128
HALO = 2
NEIGHBOURS = 3
STEPS = 10
IMAGES = 4
BEADS = 8192
NB = 8
BLOCKS = 64
N_SPACE = 8


def draw_positions(key, part):
    slabs = BEADS // BEADS_DEV
    first, second, third = jax.random.split(jax.random.fold_in(key, 11), 3)
    scales = jnp.exp(jax.random.uniform(first, (IMAGES, 1, slabs, 1), jnp.float32, 0.0, 1.39))
    noise = jnp.clip(jax.random.normal(second, (IMAGES, 3, slabs, BEADS_DEV), jnp.float32), -6.0, 6.0)
    common = 0.5 * jnp.clip(jax.random.normal(third, (1, 3, slabs, BEADS_DEV), jnp.float32), -6.0, 6.0)
    values = common + 0.5 * scales * noise
    return jnp.clip(values, -20.0, 20.0).reshape(IMAGES, 3, BEADS).astype(jnp.float32)


def draw_brackets(key, part):
    shifts = jax.random.randint(jax.random.fold_in(key, 5), (IMAGES,), -IMG_DEV, IMG_DEV, jnp.int32)
    shifts = shifts.at[IMG_DEV].set(-IMG_DEV)
    shifts = shifts.at[IMAGES - 2 * IMG_DEV].set(IMG_DEV - 1)
    centre = jnp.arange(IMAGES, dtype=jnp.int32)
    return jnp.clip(centre + shifts, 0, IMAGES - 2).astype(jnp.int32)


def with_ends(entries, key, least, high):
    shape = entries.shape
    spot = [jax.random.randint(jax.random.fold_in(key, axis), (), 0, shape[axis]) for axis in range(len(shape))]
    entries = entries.at[tuple(spot)].set(least)
    longest = shape.index(max(shape))
    spot[longest] = (spot[longest] + 1) % shape[longest]
    return entries.at[tuple(spot)].set(high)


def setup_inputs(seed: int = 0) -> dict:
    key_of = jax.random.split(jax.random.key(seed), 5)
    positions = draw_positions(jax.random.fold_in(key_of[4], 71), 0)
    neighbours = with_ends(jax.random.randint(key_of[1], (BLOCKS, NEIGHBOURS), 0, 2 * HALO + 1), jax.random.fold_in(key_of[1], 1), 0, 2 * HALO).astype(jnp.int32)
    brackets = draw_brackets(jax.random.fold_in(key_of[4], 71), 0)
    codes = with_ends(jax.random.randint(key_of[3], (IMAGES,), 0, 65536), jax.random.fold_in(key_of[3], 1), 0, 65535).astype(jnp.int32)
    return {"positions": positions, "neighbours": neighbours, "brackets": brackets, "codes": codes}


TIME_STEP = 0.05
RESTRAINT = 1.0
COUPLING = 3.0
KERNEL_RATE = 0.125
EPSILON = 1e-06
CODE_SCALE = 65536.0

def pair_forces(swarm_centres, partner_beads):
    centre_sq = lax.optimization_barrier(jnp.sum(swarm_centres * swarm_centres, axis=-3))
    partner_sq = lax.optimization_barrier(jnp.sum(partner_beads * partner_beads, axis=-3))
    crossing_flags = jnp.einsum('...euh,...euw->...uhw', swarm_centres, partner_beads, precision=lax.Precision.HIGHEST)
    weight_factors = jnp.exp(-KERNEL_RATE * (centre_sq[..., :, None] + partner_sq[..., None, :] - 2.0 * crossing_flags))
    row_sums = lax.optimization_barrier(jnp.sum(weight_factors, axis=-1))
    pulled_images = jnp.einsum('...aun,...san->...sau', weight_factors, partner_beads, precision=lax.Precision.HIGHEST)
    return COUPLING / partner_beads.shape[-1] * (swarm_centres * row_sums[..., None, :, :] - pulled_images)

def reference(positions, neighbours, brackets, codes):
    current = positions.reshape(IMAGES, 3, N_SPACE, NB, BLOCK)
    anchor = current
    bead_index = jnp.arange(NB * BLOCK, dtype=jnp.int32).reshape(NB, BLOCK)
    restrain = (bead_index < PROT_DEV).astype(jnp.float32)
    offset_table = neighbours.reshape(N_SPACE, NB, NEIGHBOURS)
    partner_blocks = (jnp.arange(NB, dtype=jnp.int32)[None, :, None] + offset_table).astype(jnp.int32)
    slab_ids = jnp.arange(N_SPACE, dtype=jnp.int32)[:, None, None]
    for turn_index in range(STEPS):
        left_rim = jnp.roll(current, 1, axis=2)[:, :, :, NB - HALO:]
        right_rim = jnp.roll(current, -1, axis=2)[:, :, :, :HALO]
        extended = jnp.concatenate([left_rim, current, right_rim], axis=3)

        def per_image(operands):
            image_ext, image_own = operands
            partner_beads = image_ext[:, slab_ids, partner_blocks]
            partner_beads = partner_beads.reshape(3, N_SPACE * NB, NEIGHBOURS * BLOCK)
            swarm_centres = image_own.reshape(3, N_SPACE * NB, BLOCK)
            return pair_forces(swarm_centres, partner_beads).reshape(3, N_SPACE, NB, BLOCK)
        forces = lax.map(per_image, (extended, current))
        current = current + TIME_STEP * (forces - RESTRAINT * restrain * (current - anchor))
    evolved = current.reshape(IMAGES, 3, N_SPACE * NB * BLOCK)
    protein = current.reshape(IMAGES, 3, N_SPACE, NB * BLOCK)[..., :PROT_DEV]
    differences = protein[1:] - protein[:-1]
    squares = lax.optimization_barrier(jnp.sum(differences * differences, axis=(1, 2, 3)))
    step_length = jnp.concatenate([jnp.zeros((1,), jnp.float32), jnp.sqrt(squares + EPSILON)])
    arc = jnp.cumsum(step_length)
    length_total = arc[IMAGES - 1]
    arc_fraction = arc / length_total
    target = (brackets.astype(jnp.float32) + codes.astype(jnp.float32) / CODE_SCALE) / (IMAGES - 1)
    arc_lower = arc[brackets]
    upper_arc_bound = arc[brackets + 1]
    weight = (target * length_total - arc_lower) / (upper_arc_bound - arc_lower)
    images_below = evolved[brackets]
    upper_images = evolved[brackets + 1]
    new_images = (1.0 - weight)[:, None, None] * images_below + weight[:, None, None] * upper_images
    return (new_images, arc_fraction)
```

```python
import functools
import math

import jax
import jax.numpy as jnp
from jax import lax
from jax.experimental import pallas as pl
from jax.experimental.pallas import tpu as pltpu
from jax.sharding import PartitionSpec as P

PROT_DEV = 128
BLOCK = 128
HALO = 2
STEPS = 10

TIME_STEP = 0.05
RESTRAINT = 1.0
COUPLING = 3.0
KERNEL_RATE = 0.125
EPSILON = 1e-06
CODE_SCALE = 65536.0

SCALE = math.sqrt(2.0 * KERNEL_RATE * math.log2(math.e))
ROWS = 8
SUB = 8
GROUP = 4


def parts_of(v):
    first = v.astype(jnp.bfloat16).astype(jnp.float32)
    rest = v - first
    second = rest.astype(jnp.bfloat16).astype(jnp.float32)
    return first, second, rest - second


def row_ids():
    return lax.broadcasted_iota(jnp.int32, (ROWS, BLOCK), 0)


def place(u, block, half, state, left_feat, right_feat, columns):
    rows = row_ids()
    u = jnp.where(rows < 3, u, 0.0)
    norm = -0.5 * jnp.sum(u * u, axis=0, keepdims=True)
    left = jnp.where(rows == 3, norm, jnp.where(rows == 4, 1.0, u))
    right = jnp.where(rows == 4, norm, jnp.where(rows == 3, 1.0, u))
    state[half, block] = u
    l1, l2, l3 = parts_of(left)
    r1, r2, r3 = parts_of(right)
    zero = jnp.zeros_like(u)
    stacked = jnp.concatenate([l1, l1, l2, l2, l1, l3, zero, zero], axis=0)
    left_feat[half, block] = stacked.T.astype(jnp.bfloat16)
    right_feat[half, block] = jnp.concatenate([r1, r2, r1, r2, r3, r1, zero, zero], axis=0).astype(jnp.bfloat16)
    tall = u.T
    for c in range(3):
        columns[half, block, c] = jnp.broadcast_to(tall[:, c : c + 1], (BLOCK, BLOCK))


def evolve_kernel(
    near, own_blocks, blocks, copies,
    table, slabs, out, shared,
    state, first, left_feat, right_feat, columns,
):
    slab = lax.axis_index("space")
    count = slabs.shape[0]
    total = count * own_blocks
    reach = HALO * STEPS

    def load(block, carry):
        spot = block + (near * own_blocks - reach)
        source = lax.rem(slab + spot // own_blocks + (count * near - near), count)
        lane = pl.multiple_of(lax.rem(spot, own_blocks) * BLOCK, BLOCK)
        x = slabs[source, :, pl.ds(lane, BLOCK)]
        u = jnp.concatenate([x * SCALE, jnp.zeros((ROWS - 3, BLOCK), jnp.float32)], axis=0)
        first[block] = u
        place(u, block, 0, state, left_feat, right_feat, columns)
        return carry

    lax.fori_loop(0, blocks, load, 0)

    def centre(block, half, last):
        row = lax.rem(slab * own_blocks + block + (total * 4 - reach), total)
        partners = table.shape[1]
        right = right_feat[half, block]
        sums = [jnp.zeros((SUB, BLOCK), jnp.float32) for _ in range(4)]
        for k in range(partners):
            other = block + table[row, k] - HALO
            power = lax.dot_general(
                left_feat[half, other], right, (((1,), (0,)), ((), ())),
                preferred_element_type=jnp.float32,
            )
            w = jnp.exp2(power)
            for r in range(0, BLOCK, SUB):
                piece = w[r : r + SUB]
                sums[3] = sums[3] + piece
                for c in range(3):
                    sums[c] = sums[c] + piece * columns[half, other, c, pl.ds(r, SUB)]
        rows = row_ids()
        sx, sy, sz, sw = [jnp.sum(s, axis=0, keepdims=True) for s in sums]
        pulled = jnp.where(rows == 0, sx, jnp.where(rows == 1, sy, sz))
        u = state[half, block]
        force = (COUPLING / (partners * BLOCK)) * (u * sw - pulled)
        spot = lax.rem(block + (own_blocks * STEPS - reach), own_blocks)
        hold = jnp.where(spot * BLOCK < PROT_DEV, RESTRAINT, 0.0)
        return u + TIME_STEP * (force - hold * (u - first[block]))

    def step(turn, carry):
        half = lax.rem(turn, 2)
        low = HALO * (turn + 1)
        groups = (blocks - 2 * low) // GROUP

        def group(index, inner):
            base = low + index * GROUP
            new = [centre(base + g, half, False) for g in range(GROUP)]
            for g in range(GROUP):
                place(new[g], base + g, 1 - half, state, left_feat, right_feat, columns)
            return inner

        lax.fori_loop(0, groups, group, 0)
        return carry

    lax.fori_loop(0, STEPS, step, 0)
    last = STEPS % 2
    for a in range(own_blocks):
        out[0, :, a * BLOCK : (a + 1) * BLOCK] = state[last, reach + a, :3] * (1.0 / SCALE)
    protein = out[0, :, :PROT_DEV]

    def spread(index, carry):
        shared[index] = protein
        return carry

    lax.fori_loop(0, copies, spread, 0)


def blend_kernel(images, slabs, brackets, codes, own, before, after, proteins, out, fraction):
    here = lax.axis_index("image")
    lower = brackets[0]
    zero = jnp.zeros((1, 1), jnp.float32)
    arcs = [zero]
    for k in range(1, images):
        d = proteins[k * slabs : (k + 1) * slabs] - proteins[(k - 1) * slabs : k * slabs]
        square = jnp.sum(jnp.sum(d * d, axis=0), axis=0, keepdims=True)
        square = jnp.sum(square, axis=1, keepdims=True)
        arcs.append(arcs[-1] + jnp.sqrt(square + EPSILON))
    total = arcs[-1]
    arc_here, arc_lower, arc_upper = zero, zero, zero
    for k in range(images):
        arc_here = jnp.where(here == k, arcs[k], arc_here)
        arc_lower = jnp.where(lower == k, arcs[k], arc_lower)
        arc_upper = jnp.where(lower + 1 == k, arcs[k], arc_upper)
    base = jnp.full((1, 1), lower, jnp.int32).astype(jnp.float32)
    code = jnp.full((1, 1), codes[0], jnp.int32).astype(jnp.float32)
    target = (base + code / CODE_SCALE) / (images - 1)
    weight = (target * total - arc_lower) / (arc_upper - arc_lower)
    mine, previous, following = own[0], before[0], after[0]
    below = jnp.where(lower == here, mine, previous)
    above = jnp.where(lower == here, following, mine)
    out[0] = (1.0 - weight) * below + weight * above
    fraction[...] = arc_here / total


def body(positions, neighbours, brackets, codes):
    slab_beads = positions.shape[2]
    own_blocks = slab_beads // BLOCK
    slabs = lax.axis_size("space")
    images = lax.axis_size("image")
    devices = slabs * images
    reach = HALO * STEPS
    blocks = own_blocks + 2 * reach
    near = -(-reach // own_blocks)
    vmem = pl.BlockSpec(memory_space=pltpu.VMEM)
    smem = pl.BlockSpec(memory_space=pltpu.SMEM)
    spread = jnp.broadcast_to(positions, (slabs,) + positions.shape[1:])
    around = lax.all_to_all(spread, "space", 0, 0, tiled=True)
    evolved, shared = pl.pallas_call(
        functools.partial(evolve_kernel, near, own_blocks, blocks, devices),
        out_shape=(
            jax.ShapeDtypeStruct(positions.shape, jnp.float32),
            jax.ShapeDtypeStruct((devices, 3, PROT_DEV), jnp.float32),
        ),
        in_specs=[smem, vmem],
        out_specs=(vmem, vmem),
        scratch_shapes=[
            pltpu.VMEM((2, blocks, ROWS, BLOCK), jnp.float32),
            pltpu.VMEM((blocks, ROWS, BLOCK), jnp.float32),
            pltpu.VMEM((2, blocks, BLOCK, 8 * ROWS), jnp.bfloat16),
            pltpu.VMEM((2, blocks, 8 * ROWS, BLOCK), jnp.bfloat16),
            pltpu.VMEM((2, blocks, 3, BLOCK, BLOCK), jnp.float32),
        ],
    )(neighbours, around)
    up = [(i, i + 1) for i in range(images - 1)]
    down = [(i + 1, i) for i in range(images - 1)]
    proteins = lax.all_to_all(shared, ("image", "space"), 0, 0, tiled=True)
    before = lax.ppermute(evolved, "image", up)
    after = lax.ppermute(evolved, "image", down)
    new_images, fraction = pl.pallas_call(
        functools.partial(blend_kernel, images, slabs),
        out_shape=(
            jax.ShapeDtypeStruct(positions.shape, jnp.float32),
            jax.ShapeDtypeStruct((1, 1), jnp.float32),
        ),
        in_specs=[smem, smem, vmem, vmem, vmem, vmem],
        out_specs=(vmem, vmem),
    )(brackets, codes, evolved, before, after, proteins)
    return new_images, fraction.reshape(1)


def solution(mesh):
    placed = (P("image", None, "space"), P(), P("image"), P("image"))
    return jax.shard_map(
        body,
        mesh=mesh,
        in_specs=placed,
        out_specs=(P("image", None, "space"), P("image")),
        check_vma=False,
    )
```

```python
import functools
import math

import jax
import jax.numpy as jnp
from jax import lax
from jax.experimental import pallas as pl
from jax.experimental.pallas import tpu as pltpu
from jax.sharding import PartitionSpec as P

PROT_DEV = 128
BLOCK = 128
HALO = 2
STEPS = 10

TIME_STEP = 0.05
RESTRAINT = 1.0
COUPLING = 3.0
KERNEL_RATE = 0.125
EPSILON = 1e-06
CODE_SCALE = 65536.0

SCALE = math.sqrt(2.0 * KERNEL_RATE * math.log2(math.e))
ROWS = 8
SUB = 8
GROUP = 4
PAD = GROUP
PHASES = (6, 4)


def parts_of(v):
    first = v.astype(jnp.bfloat16).astype(jnp.float32)
    rest = v - first
    second = rest.astype(jnp.bfloat16).astype(jnp.float32)
    return first, second, rest - second


def row_ids():
    return lax.broadcasted_iota(jnp.int32, (ROWS, BLOCK), 0)


def spread_matrix():
    row = lax.broadcasted_iota(jnp.int32, (8 * ROWS, 3 * BLOCK), 0)
    column = lax.broadcasted_iota(jnp.int32, (8 * ROWS, 3 * BLOCK), 1) // BLOCK
    chosen = (row == column) | (row == column + 2 * ROWS) | (row == column + 5 * ROWS)
    return jnp.where(chosen, 1.0, 0.0).astype(jnp.bfloat16)


def place(u, block, refs, picks):
    state, left_feat, right_feat, columns = refs
    rows = row_ids()
    u = jnp.where(rows < 3, u, 0.0)
    norm = -0.5 * jnp.sum(u * u, axis=0, keepdims=True)
    left = jnp.where(rows == 3, norm, jnp.where(rows == 4, 1.0, u))
    right = jnp.where(rows == 4, norm, jnp.where(rows == 3, 1.0, u))
    state[block] = u
    l1, l2, l3 = parts_of(left)
    r1, r2, r3 = parts_of(right)
    zero = jnp.zeros_like(u)
    stacked = jnp.concatenate([l1, l1, l2, l2, l1, l3, zero, zero], axis=0)
    tall = stacked.T.astype(jnp.bfloat16)
    left_feat[block] = tall
    right_feat[block] = jnp.concatenate([r1, r2, r1, r2, r3, r1, zero, zero], axis=0).astype(jnp.bfloat16)
    columns[block] = lax.dot_general(
        tall, picks[...], (((1,), (0,)), ((), ())), preferred_element_type=jnp.float32
    )


def evolve_kernel(
    steps, near, copies, table, *refs,
):
    slabs, refs = refs[: 2 * near + 1], refs[2 * near + 1 :]
    if copies:
        anchors, refs = refs[: 2 * near + 1], refs[2 * near + 1 :]
        out, shared, refs = refs[0], refs[1], refs[2:]
    else:
        anchors, out, refs = slabs, refs[0], refs[1:]
    first, picks, even, odd = refs[0], refs[1], refs[2:6], refs[6:]
    own_blocks = out.shape[1]
    partners = table.shape[0]
    total = table.shape[1]
    reach = HALO * steps
    blocks = own_blocks + 2 * reach
    slab = lax.axis_index("space")
    picks[...] = spread_matrix()
    filler = jnp.zeros((ROWS - 3, BLOCK), jnp.float32)

    def scaled(ref, block):
        return jnp.concatenate([ref[:, block, :] * SCALE, filler], axis=0)

    for index in range(2 * near + 1):
        shift = (index - near) * own_blocks + reach
        begin, end = max(0, -shift), min(own_blocks, blocks - shift)

        def load(turn, carry, index=index, begin=begin, shift=shift):
            for g in range(GROUP):
                block = begin + turn * GROUP + g
                first[block + shift + PAD] = scaled(anchors[index], block)
                place(scaled(slabs[index], block), block + shift + PAD, even, picks)
            return carry

        lax.fori_loop(0, (end - begin) // GROUP, load, 0)

    def centre(block, source):
        state, left_feat, right_feat, columns = source
        spot = block - (PAD + reach)
        row = lax.rem(slab * own_blocks + spot + total, total)
        right = right_feat[block]
        sums = [jnp.zeros((SUB, BLOCK), jnp.float32) for _ in range(4)]
        for k in range(partners):
            other = block + table[k, row] - HALO
            power = lax.dot_general(
                left_feat[other], right, (((1,), (0,)), ((), ())),
                preferred_element_type=jnp.float32,
            )
            w = jnp.exp2(power)
            for r in range(0, BLOCK, SUB):
                piece = w[r : r + SUB]
                sums[3] = sums[3] + piece
                for c in range(3):
                    sums[c] = sums[c] + piece * columns[other, pl.ds(r, SUB), c * BLOCK : (c + 1) * BLOCK]
        rows = row_ids()
        sx, sy, sz, sw = [jnp.sum(s, axis=0, keepdims=True) for s in sums]
        pulled = jnp.where(rows == 0, sx, jnp.where(rows == 1, sy, sz))
        u = state[block]
        force = (COUPLING / (partners * BLOCK)) * (u * sw - pulled)
        inner = lax.rem(spot + own_blocks * near, own_blocks)
        hold = jnp.where(inner * BLOCK < PROT_DEV, RESTRAINT, 0.0)
        return u + TIME_STEP * (force - hold * (u - first[block]))

    def step(turn, source, target, final=False):
        low = HALO * (turn + 1) + PAD
        groups = (blocks + 2 * PAD - 2 * low) // GROUP

        def keep(new, base):
            for g in range(GROUP):
                if final:
                    target[0][base + g] = new[g]
                else:
                    place(new[g], base + g, target, picks)

        def group(index, held):
            base = low + index * GROUP
            keep(held, base - GROUP)
            return tuple(centre(base + g, source) for g in range(GROUP))

        start = tuple(jnp.zeros((ROWS, BLOCK), jnp.float32) for _ in range(GROUP))
        held = lax.fori_loop(0, groups, group, start)
        keep(held, low + (groups - 1) * GROUP)

    def both(pair, carry):
        step(2 * pair, even, odd)
        step(2 * pair + 1, odd, even)
        return carry

    lax.fori_loop(0, steps // 2 - 1, both, 0)
    step(steps - 2, even, odd)
    step(steps - 1, odd, even, True)
    for a in range(own_blocks):
        out[:, a, :] = even[0][PAD + reach + a, :3] * (1.0 / SCALE)
    if copies:
        protein = out[:, 0, :]

        def spread(index, carry):
            shared[index] = protein
            return carry

        lax.fori_loop(0, copies, spread, 0)


def blend_kernel(images, slabs, brackets, codes, own, before, after, proteins, out, fraction):
    here = lax.axis_index("image")
    lower = brackets[0]
    zero = jnp.zeros((1, 1), jnp.float32)
    arcs = [zero]
    for k in range(1, images):
        d = proteins[k * slabs : (k + 1) * slabs] - proteins[(k - 1) * slabs : k * slabs]
        square = jnp.sum(jnp.sum(d * d, axis=0), axis=0, keepdims=True)
        square = jnp.sum(square, axis=1, keepdims=True)
        arcs.append(arcs[-1] + jnp.sqrt(square + EPSILON))
    total = arcs[-1]
    arc_here, arc_lower, arc_upper = zero, zero, zero
    for k in range(images):
        arc_here = jnp.where(here == k, arcs[k], arc_here)
        arc_lower = jnp.where(lower == k, arcs[k], arc_lower)
        arc_upper = jnp.where(lower + 1 == k, arcs[k], arc_upper)
    base = jnp.full((1, 1), lower, jnp.int32).astype(jnp.float32)
    code = jnp.full((1, 1), codes[0], jnp.int32).astype(jnp.float32)
    target = (base + code / CODE_SCALE) / (images - 1)
    weight = (target * total - arc_lower) / (arc_upper - arc_lower)
    mine, previous, following = own[...], before[...], after[...]
    below = jnp.where(lower == here, mine, previous)
    above = jnp.where(lower == here, following, mine)
    weight = jnp.reshape(weight, (1, 1, 1))
    out[...] = (1.0 - weight) * below + weight * above
    fraction[...] = arc_here / total


VMEM = pl.BlockSpec(memory_space=pltpu.VMEM)
SMEM = pl.BlockSpec(memory_space=pltpu.SMEM)


def around(cells, near):
    count = lax.axis_size("space")
    found = []
    for distance in range(-near, near + 1):
        route = [((i + distance) % count, i) for i in range(count)]
        found.append(lax.ppermute(cells, "space", route) if distance else cells)
    return found


def evolve(steps, copies, table, slabs, anchors):
    shape = slabs[0].shape
    near = len(slabs) // 2
    blocks = shape[1] + 2 * HALO * steps + 2 * PAD
    outs = [jax.ShapeDtypeStruct(shape, jnp.float32)]
    if copies:
        outs.append(jax.ShapeDtypeStruct((copies, 3, PROT_DEV), jnp.float32))
    half = [
        pltpu.VMEM((blocks, ROWS, BLOCK), jnp.float32),
        pltpu.VMEM((blocks, BLOCK, 8 * ROWS), jnp.bfloat16),
        pltpu.VMEM((blocks, 8 * ROWS, BLOCK), jnp.bfloat16),
        pltpu.VMEM((blocks, BLOCK, 3 * BLOCK), jnp.float32),
    ]
    return pl.pallas_call(
        functools.partial(evolve_kernel, steps, near, copies),
        out_shape=outs,
        in_specs=[SMEM] + [VMEM] * (len(slabs) + len(anchors)),
        out_specs=[VMEM] * len(outs),
        scratch_shapes=[
            pltpu.VMEM((blocks, ROWS, BLOCK), jnp.float32),
            pltpu.VMEM((8 * ROWS, 3 * BLOCK), jnp.bfloat16),
            *half,
            *half,
        ],
        compiler_params=pltpu.CompilerParams(vmem_limit_bytes=32 << 20),
    )(table, *slabs, *anchors)


def body(positions, neighbours, brackets, codes):
    slabs = lax.axis_size("space")
    images = lax.axis_size("image")
    own_blocks = positions.shape[2] // BLOCK
    cells = positions.reshape(3, own_blocks, BLOCK)
    table = neighbours.T
    first = around(cells, -(-HALO * PHASES[0] // own_blocks))
    (middle,) = evolve(PHASES[0], 0, table, first, [])
    near = -(-HALO * PHASES[1] // own_blocks)
    skip = len(first) // 2 - near
    anchors = first[skip : len(first) - skip]
    evolved, shared = evolve(PHASES[1], slabs * images, table, around(middle, near), anchors)
    up = [(i, i + 1) for i in range(images - 1)]
    down = [(i + 1, i) for i in range(images - 1)]
    proteins = lax.all_to_all(shared, ("image", "space"), 0, 0, tiled=True)
    before = lax.ppermute(evolved, "image", up)
    after = lax.ppermute(evolved, "image", down)
    new_images, fraction = pl.pallas_call(
        functools.partial(blend_kernel, images, slabs),
        out_shape=(
            jax.ShapeDtypeStruct(cells.shape, jnp.float32),
            jax.ShapeDtypeStruct((1, 1), jnp.float32),
        ),
        in_specs=[SMEM, SMEM, VMEM, VMEM, VMEM, VMEM],
        out_specs=(VMEM, VMEM),
        compiler_params=pltpu.CompilerParams(vmem_limit_bytes=8 << 20),
    )(brackets, codes, evolved, before, after, proteins)
    return new_images.reshape(positions.shape), fraction.reshape(1)


def solution(mesh):
    placed = (P("image", None, "space"), P(), P("image"), P("image"))
    return jax.shard_map(
        body,
        mesh=mesh,
        in_specs=placed,
        out_specs=(P("image", None, "space"), P("image")),
        check_vma=False,
    )
```

```python
import functools
import math

import jax
import jax.numpy as jnp
from jax import lax
from jax.experimental import pallas as pl
from jax.experimental.pallas import tpu as pltpu
from jax.sharding import PartitionSpec as P

PROT_DEV = 128
BLOCK = 128
HALO = 2
STEPS = 10

TIME_STEP = 0.05
RESTRAINT = 1.0
COUPLING = 3.0
KERNEL_RATE = 0.125
EPSILON = 1e-06
CODE_SCALE = 65536.0

SCALE = math.sqrt(2.0 * KERNEL_RATE * math.log2(math.e))
ROWS = 8
SUB = 8
GROUP = 4
PAD = GROUP
HALF = 8 * ROWS
WIDTH = 2 * HALF
PHASES = (6, 4)


def parts_of(v):
    first = v.astype(jnp.bfloat16).astype(jnp.float32)
    rest = v - first
    second = rest.astype(jnp.bfloat16).astype(jnp.float32)
    return first, second, rest - second


def row_ids():
    return lax.broadcasted_iota(jnp.int32, (ROWS, BLOCK), 0)


def spread_matrices():
    row = lax.broadcasted_iota(jnp.int32, (WIDTH, 2 * BLOCK), 0)
    column = lax.broadcasted_iota(jnp.int32, (WIDTH, 2 * BLOCK), 1) // BLOCK

    def picked(inner, component):
        return (inner == component) | (inner == component + 2 * ROWS) | (inner == component + 5 * ROWS)

    plane = picked(row, column)
    depth = picked(row - HALF * column, 2)
    return [jnp.where(chosen, 1.0, 0.0).astype(jnp.bfloat16) for chosen in (plane, depth)]


def multiply(left, right):
    return lax.dot_general(left, right, (((1,), (0,)), ((), ())), preferred_element_type=jnp.float32)


def side_by_side(low, high):
    lane = lax.broadcasted_iota(jnp.int32, (BLOCK, WIDTH), 1)
    return jnp.where(lane < HALF, low, high)


def place(new, base, refs, picks):
    state, left_feat, right_feat, columns = refs
    rows = row_ids()
    talls = []
    for g, u in enumerate(new):
        u = jnp.where(rows < 3, u, 0.0)
        norm = -0.5 * jnp.sum(u * u, axis=0, keepdims=True)
        left = jnp.where(rows == 3, norm, jnp.where(rows == 4, 1.0, u))
        right = jnp.where(rows == 4, norm, jnp.where(rows == 3, 1.0, u))
        state[base + g] = u
        l1, l2, l3 = parts_of(left)
        r1, r2, r3 = parts_of(right)
        zero = jnp.zeros_like(u)
        stacked = [l1, l1, l2, l2, l1, l3, zero, zero]
        tall = jnp.concatenate(stacked + stacked, axis=0).T.astype(jnp.bfloat16)
        left_feat[base + g] = tall
        right_feat[base + g] = jnp.concatenate([r1, r2, r1, r2, r3, r1, zero, zero], axis=0).astype(jnp.bfloat16)
        columns[base + g, :, : 2 * BLOCK] = multiply(tall, picks[0])
        talls.append(tall)
    for g in range(0, len(new), 2):
        depth = multiply(side_by_side(talls[g], talls[g + 1]), picks[1])
        columns[base + g, :, 2 * BLOCK :] = depth[:, :BLOCK]
        columns[base + g + 1, :, 2 * BLOCK :] = depth[:, BLOCK:]


def evolve_kernel(
    steps, near, copies, table, *refs,
):
    slabs, refs = refs[: 2 * near + 1], refs[2 * near + 1 :]
    if copies:
        anchors, refs = refs[: 2 * near + 1], refs[2 * near + 1 :]
        out, shared, refs = refs[0], refs[1], refs[2:]
    else:
        anchors, out, refs = slabs, refs[0], refs[1:]
    first, picks, weights, even, odd = refs[0], refs[1], refs[2], refs[3:7], refs[7:]
    own_blocks = out.shape[1]
    partners = table.shape[0]
    total = table.shape[1]
    reach = HALO * steps
    blocks = own_blocks + 2 * reach
    slab = lax.axis_index("space")
    picks[0], picks[1] = spread_matrices()
    filler = jnp.zeros((ROWS - 3, BLOCK), jnp.float32)

    def scaled(ref, block):
        return jnp.concatenate([ref[:, block, :] * SCALE, filler], axis=0)

    for index in range(2 * near + 1):
        shift = (index - near) * own_blocks + reach
        begin, end = max(0, -shift), min(own_blocks, blocks - shift)

        def load(turn, carry, index=index, begin=begin, shift=shift):
            block = begin + turn * GROUP
            for g in range(GROUP):
                first[block + g + shift + PAD] = scaled(anchors[index], block + g)
            new = [scaled(slabs[index], block + g) for g in range(GROUP)]
            place(new, block + shift + PAD, even, picks)
            return carry

        lax.fori_loop(0, (end - begin) // GROUP, load, 0)

    def start_of(block):
        return lax.rem(slab * own_blocks + (block - (PAD + reach)) + total, total)

    def other_of(block, k):
        return block + table[k, start_of(block)] - HALO

    def powers(base, source):
        _, left_feat, right_feat, _ = source
        blank = jnp.zeros((HALF, BLOCK), jnp.bfloat16)
        found = []
        for block in [base + g for g in range(0, GROUP, 2)]:
            right = jnp.concatenate([
                jnp.concatenate([right_feat[block], blank], axis=1),
                jnp.concatenate([blank, right_feat[block + 1]], axis=1),
            ], axis=0)
            found.append([
                multiply(side_by_side(left_feat[other_of(block, k)], left_feat[other_of(block + 1, k)]), right)
                for k in range(partners)
            ])
        return found

    def keep_weights(found):
        for p, row in enumerate(found):
            for k, power in enumerate(row):
                weights[p, k] = jnp.exp2(power)

    def advance(base, source):
        state, _, _, columns = source
        rows = row_ids()
        found = []
        for g in range(GROUP):
            block = base + g
            sums = [jnp.zeros((SUB, BLOCK), jnp.float32) for _ in range(4)]
            lane = (g % 2) * BLOCK
            for k in range(partners):
                other = other_of(block, k)
                for r in range(0, BLOCK, SUB):
                    piece = weights[g // 2, k, r : r + SUB, lane : lane + BLOCK]
                    sums[3] = sums[3] + piece
                    for c in range(3):
                        sums[c] = sums[c] + piece * columns[other, r : r + SUB, c * BLOCK : (c + 1) * BLOCK]
            sx, sy, sz, sw = [jnp.sum(s, axis=0, keepdims=True) for s in sums]
            pulled = jnp.where(rows == 0, sx, jnp.where(rows == 1, sy, sz))
            u = state[block]
            force = (COUPLING / (partners * BLOCK)) * (u * sw - pulled)
            inner = lax.rem(block - (PAD + reach) + own_blocks * near, own_blocks)
            hold = jnp.where(inner * BLOCK < PROT_DEV, RESTRAINT, 0.0)
            found.append(u + TIME_STEP * (force - hold * (u - first[block])))
        return tuple(found)

    def turn(ask, move, store, held):
        found = powers(*ask) if ask else None
        new = advance(*move) if move else held
        if ask:
            keep_weights(found)
        if store:
            base, target = store
            if target is None:
                for g in range(GROUP):
                    even[0][base + g] = held[g]
            else:
                place(held, base, target, picks)
        return new

    halves = (even, odd)
    last = None
    for t in range(steps):
        source, target = halves[t % 2], halves[1 - t % 2] if t < steps - 1 else None
        low = HALO * (t + 1) + PAD
        count = (blocks + 2 * PAD - 2 * low) // GROUP

        def at(g, refs, low=low):
            return low + g * GROUP, refs

        if t == 0:
            turn(at(0, source), None, None, None)
            held = turn(at(1, source), at(0, source), None, None)
        elif last[0] < 4:
            tail = turn(None, last[1](last[0] - 1, last[2]), last[1](last[0] - 2, last[3]), held)
            turn(at(0, source), None, last[1](last[0] - 1, last[3]), tail)
            held = turn(at(1, source), at(0, source), None, None)
        else:
            held = turn(at(0, source), last[1](last[0] - 1, last[2]), last[1](last[0] - 2, last[3]), held)
            held = turn(at(1, source), at(0, source), last[1](last[0] - 1, last[3]), held)

        def steady(g, held, at=at, source=source, target=target):
            return turn(at(g, source), at(g - 1, source), at(g - 2, target), held)

        held = lax.fori_loop(2, count, steady, held)
        last = (count, at, source, target)
    tail = turn(None, last[1](last[0] - 1, last[2]), last[1](last[0] - 2, None), held)
    turn(None, None, last[1](last[0] - 1, None), tail)
    for a in range(own_blocks):
        out[:, a, :] = even[0][PAD + reach + a, :3] * (1.0 / SCALE)
    if copies:
        protein = out[:, 0, :]

        def spread(index, carry):
            shared[index] = protein
            return carry

        lax.fori_loop(0, copies, spread, 0)


def blend_kernel(images, slabs, brackets, codes, own, before, after, proteins, out, fraction):
    here = lax.axis_index("image")
    lower = brackets[0]
    zero = jnp.zeros((1, 1), jnp.float32)
    arcs = [zero]
    for k in range(1, images):
        d = proteins[k * slabs : (k + 1) * slabs] - proteins[(k - 1) * slabs : k * slabs]
        square = jnp.sum(jnp.sum(d * d, axis=0), axis=0, keepdims=True)
        square = jnp.sum(square, axis=1, keepdims=True)
        arcs.append(arcs[-1] + jnp.sqrt(square + EPSILON))
    total = arcs[-1]
    arc_here, arc_lower, arc_upper = zero, zero, zero
    for k in range(images):
        arc_here = jnp.where(here == k, arcs[k], arc_here)
        arc_lower = jnp.where(lower == k, arcs[k], arc_lower)
        arc_upper = jnp.where(lower + 1 == k, arcs[k], arc_upper)
    base = jnp.full((1, 1), lower, jnp.int32).astype(jnp.float32)
    code = jnp.full((1, 1), codes[0], jnp.int32).astype(jnp.float32)
    target = (base + code / CODE_SCALE) / (images - 1)
    weight = (target * total - arc_lower) / (arc_upper - arc_lower)
    mine, previous, following = own[...], before[...], after[...]
    below = jnp.where(lower == here, mine, previous)
    above = jnp.where(lower == here, following, mine)
    weight = jnp.reshape(weight, (1, 1, 1))
    out[...] = (1.0 - weight) * below + weight * above
    fraction[...] = arc_here / total


VMEM = pl.BlockSpec(memory_space=pltpu.VMEM)
SMEM = pl.BlockSpec(memory_space=pltpu.SMEM)


def around(cells, near):
    count = lax.axis_size("space")
    found = []
    for distance in range(-near, near + 1):
        route = [((i + distance) % count, i) for i in range(count)]
        found.append(lax.ppermute(cells, "space", route) if distance else cells)
    return found


def evolve(steps, copies, table, slabs, anchors):
    shape = slabs[0].shape
    near = len(slabs) // 2
    blocks = shape[1] + 2 * HALO * steps + 2 * PAD
    outs = [jax.ShapeDtypeStruct(shape, jnp.float32)]
    if copies:
        outs.append(jax.ShapeDtypeStruct((copies, 3, PROT_DEV), jnp.float32))
    half = [
        pltpu.VMEM((blocks, ROWS, BLOCK), jnp.float32),
        pltpu.VMEM((blocks, BLOCK, WIDTH), jnp.bfloat16),
        pltpu.VMEM((blocks, HALF, BLOCK), jnp.bfloat16),
        pltpu.VMEM((blocks, BLOCK, 3 * BLOCK), jnp.float32),
    ]
    return pl.pallas_call(
        functools.partial(evolve_kernel, steps, near, copies),
        out_shape=outs,
        in_specs=[SMEM] + [VMEM] * (len(slabs) + len(anchors)),
        out_specs=[VMEM] * len(outs),
        scratch_shapes=[
            pltpu.VMEM((blocks, ROWS, BLOCK), jnp.float32),
            pltpu.VMEM((2, WIDTH, 2 * BLOCK), jnp.bfloat16),
            pltpu.VMEM((GROUP // 2, table.shape[0], BLOCK, 2 * BLOCK), jnp.float32),
            *half,
            *half,
        ],
        compiler_params=pltpu.CompilerParams(vmem_limit_bytes=32 << 20),
    )(table, *slabs, *anchors)


def body(positions, neighbours, brackets, codes):
    slabs = lax.axis_size("space")
    images = lax.axis_size("image")
    own_blocks = positions.shape[2] // BLOCK
    cells = positions.reshape(3, own_blocks, BLOCK)
    table = neighbours.T
    first = around(cells, -(-HALO * PHASES[0] // own_blocks))
    (middle,) = evolve(PHASES[0], 0, table, first, [])
    near = -(-HALO * PHASES[1] // own_blocks)
    skip = len(first) // 2 - near
    anchors = first[skip : len(first) - skip]
    evolved, shared = evolve(PHASES[1], slabs * images, table, around(middle, near), anchors)
    up = [(i, i + 1) for i in range(images - 1)]
    down = [(i + 1, i) for i in range(images - 1)]
    proteins = lax.all_to_all(shared, ("image", "space"), 0, 0, tiled=True)
    before = lax.ppermute(evolved, "image", up)
    after = lax.ppermute(evolved, "image", down)
    new_images, fraction = pl.pallas_call(
        functools.partial(blend_kernel, images, slabs),
        out_shape=(
            jax.ShapeDtypeStruct(cells.shape, jnp.float32),
            jax.ShapeDtypeStruct((1, 1), jnp.float32),
        ),
        in_specs=[SMEM, SMEM, VMEM, VMEM, VMEM, VMEM],
        out_specs=(VMEM, VMEM),
        compiler_params=pltpu.CompilerParams(vmem_limit_bytes=8 << 20),
    )(brackets, codes, evolved, before, after, proteins)
    return new_images.reshape(positions.shape), fraction.reshape(1)


def solution(mesh):
    placed = (P("image", None, "space"), P(), P("image"), P("image"))
    return jax.shard_map(
        body,
        mesh=mesh,
        in_specs=placed,
        out_specs=(P("image", None, "space"), P("image")),
        check_vma=False,
    )
```

```python
import functools
import math

import jax
import jax.numpy as jnp
from jax import lax
from jax.experimental import pallas as pl
from jax.experimental.pallas import tpu as pltpu
from jax.sharding import PartitionSpec as P

PROT_DEV = 128
BLOCK = 128
HALO = 2
STEPS = 10

TIME_STEP = 0.05
RESTRAINT = 1.0
COUPLING = 3.0
KERNEL_RATE = 0.125
EPSILON = 1e-06
CODE_SCALE = 65536.0

SCALE = math.sqrt(2.0 * KERNEL_RATE * math.log2(math.e))
ROWS = 8
SUB = 8
GROUP = 4
LOAD_GROUP = 8
PAD = GROUP
HALF = 8 * ROWS
WIDTH = 2 * HALF
PHASES = (6, 4)


def parts_of(v):
    first = v.astype(jnp.bfloat16).astype(jnp.float32)
    rest = v - first
    second = rest.astype(jnp.bfloat16).astype(jnp.float32)
    return first, second, rest - second


def row_ids():
    return lax.broadcasted_iota(jnp.int32, (ROWS, BLOCK), 0)


def spread_matrices():
    row = lax.broadcasted_iota(jnp.int32, (WIDTH, 2 * BLOCK), 0)
    column = lax.broadcasted_iota(jnp.int32, (WIDTH, 2 * BLOCK), 1) // BLOCK

    def picked(inner, component):
        return (inner == component) | (inner == component + 2 * ROWS) | (inner == component + 5 * ROWS)

    plane = picked(row, column)
    depth = picked(row - HALF * column, 2)
    return [jnp.where(chosen, 1.0, 0.0).astype(jnp.bfloat16) for chosen in (plane, depth)]


def multiply(left, right):
    return lax.dot_general(left, right, (((1,), (0,)), ((), ())), preferred_element_type=jnp.float32)


def side_by_side(low, high):
    lane = lax.broadcasted_iota(jnp.int32, (BLOCK, WIDTH), 1)
    return jnp.where(lane < HALF, low, high)


def place(new, base, refs, picks):
    state, left_feat, right_feat, columns = refs
    rows = row_ids()
    talls = []
    for g, u in enumerate(new):
        u = jnp.where(rows < 3, u, 0.0)
        norm = -0.5 * jnp.sum(u * u, axis=0, keepdims=True)
        left = jnp.where(rows == 3, norm, jnp.where(rows == 4, 1.0, u))
        right = jnp.where(rows == 4, norm, jnp.where(rows == 3, 1.0, u))
        state[base + g] = u
        l1, l2, l3 = parts_of(left)
        r1, r2, r3 = parts_of(right)
        zero = jnp.zeros_like(u)
        stacked = [l1, l1, l2, l2, l1, l3, zero, zero]
        tall = jnp.concatenate(stacked + stacked, axis=0).T.astype(jnp.bfloat16)
        left_feat[base + g] = tall
        right_feat[base + g] = jnp.concatenate([r1, r2, r1, r2, r3, r1, zero, zero], axis=0).astype(jnp.bfloat16)
        columns[base + g, :, : 2 * BLOCK] = multiply(tall, picks[0])
        columns[base + g, :, 2 * BLOCK :] = jnp.broadcast_to(u.T[:, 2:3], (BLOCK, BLOCK))


def evolve_kernel(
    steps, near, copies, table, *refs,
):
    slabs, refs = refs[: 2 * near + 1], refs[2 * near + 1 :]
    if copies:
        anchors, refs = refs[: 2 * near + 1], refs[2 * near + 1 :]
        out, shared, refs = refs[0], refs[1], refs[2:]
    else:
        anchors, out, refs = slabs, refs[0], refs[1:]
    first, picks, others, weights, even, odd = refs[0], refs[1], refs[2], refs[3], refs[4:8], refs[8:]
    own_blocks = out.shape[1]
    partners = table.shape[0]
    total = table.shape[1]
    reach = HALO * steps
    blocks = own_blocks + 2 * reach
    slab = lax.axis_index("space")
    slabs_around = total // own_blocks
    picks[0], picks[1] = spread_matrices()
    filler = jnp.zeros((ROWS - 3, BLOCK), jnp.float32)

    def scaled(ref, block, ready):
        x = ref[:, block, :]
        return jnp.concatenate([x if ready else x * SCALE, filler], axis=0)

    for index in range(2 * near + 1):
        shift = (index - near) * own_blocks + reach
        begin, end = max(0, -shift), min(own_blocks, blocks - shift)
        size = LOAD_GROUP if (end - begin) % LOAD_GROUP == 0 else GROUP

        def load(turn, carry, index=index, begin=begin, shift=shift, size=size):
            block = begin + turn * size
            for g in range(size):
                spot = block + g + shift + PAD
                first[spot] = scaled(anchors[index], block + g, index == near)
                row = lax.rem((slab + index - near + slabs_around) * own_blocks + block + g, total)
                for k in range(partners):
                    others[spot * partners + k] = spot + table[k, row] - HALO
            new = [scaled(slabs[index], block + g, copies or index == near) for g in range(size)]
            place(new, block + shift + PAD, even, picks)
            return carry

        lax.fori_loop(0, (end - begin) // size, load, 0)
    for spot in [*range(PAD), *range(PAD + blocks, 2 * PAD + blocks)]:
        for k in range(partners):
            others[spot * partners + k] = PAD

    def partners_of(base):
        spot = base * partners
        return tuple(tuple(others[spot + (g * partners + k)] for k in range(partners)) for g in range(GROUP))

    def powers(base, source, near_blocks, p):
        _, left_feat, right_feat, _ = source
        blank = jnp.zeros((HALF, BLOCK), jnp.bfloat16)
        found = []
        for g in (2 * p,):
            block = base + g
            right = jnp.concatenate([
                jnp.concatenate([right_feat[block], blank], axis=1),
                jnp.concatenate([blank, blank], axis=1),
                jnp.concatenate([blank, right_feat[block + 1]], axis=1),
                jnp.concatenate([blank, blank], axis=1),
            ], axis=0)
            found.append([
                multiply(jnp.concatenate([left_feat[near_blocks[g][k]], left_feat[near_blocks[g + 1][k]]], axis=1), right)
                for k in range(partners)
            ])
        return found

    def keep_weights(found, p):
        for k, power in enumerate(found[0]):
            weights[p, k] = jnp.exp2(power)

    def advance(base, source, near_blocks, p):
        state, _, _, columns = source
        rows = row_ids()
        found = []
        for g in (2 * p, 2 * p + 1):
            block = base + g
            sums = [jnp.zeros((SUB, BLOCK), jnp.float32) for _ in range(4)]
            lane = (g % 2) * BLOCK
            for k in range(partners):
                other = near_blocks[g][k]
                for r in range(0, BLOCK, SUB):
                    piece = weights[g // 2, k, r : r + SUB, lane : lane + BLOCK]
                    sums[3] = sums[3] + piece
                    for c in range(3):
                        sums[c] = sums[c] + piece * columns[other, r : r + SUB, c * BLOCK : (c + 1) * BLOCK]
            sx, sy, sz, sw = [jnp.sum(s, axis=0, keepdims=True) for s in sums]
            pulled = jnp.where(rows == 0, sx, jnp.where(rows == 1, sy, sz))
            u = state[block]
            force = (COUPLING / (partners * BLOCK)) * (u * sw - pulled)
            inner = lax.rem(block - (PAD + reach) + own_blocks * near, own_blocks)
            hold = jnp.where(inner * BLOCK < PROT_DEV, RESTRAINT, 0.0)
            found.append(u + TIME_STEP * (force - hold * (u - first[block])))
        return tuple(found)

    def turn(ask, move, store, carried):
        held, near_blocks = carried
        asked = partners_of(ask[0]) if ask else None
        new = () if move else held
        for p in range(GROUP // 2):
            found = powers(*ask, asked, p) if ask else None
            if move:
                new += advance(*move, near_blocks, p)
            if ask:
                keep_weights(found, p)
            if store:
                base, target = store
                if target is None:
                    for g in (2 * p, 2 * p + 1):
                        even[0][base + g] = held[g]
                else:
                    place(held[2 * p : 2 * p + 2], base + 2 * p, target, picks)
        return new, asked

    halves = (even, odd)
    last = None
    for t in range(steps):
        source, target = halves[t % 2], halves[1 - t % 2] if t < steps - 1 else None
        low = HALO * (t + 1) + PAD
        count = (blocks + 2 * PAD - 2 * low) // GROUP

        def at(g, refs, low=low):
            return low + g * GROUP, refs

        if t == 0:
            held = turn(at(0, source), None, None, (None, None))
            held = turn(at(1, source), at(0, source), None, held)
        elif last[0] < 4:
            tail = turn(None, last[1](last[0] - 1, last[2]), last[1](last[0] - 2, last[3]), held)
            held = turn(at(0, source), None, last[1](last[0] - 1, last[3]), tail)
            held = turn(at(1, source), at(0, source), None, held)
        else:
            held = turn(at(0, source), last[1](last[0] - 1, last[2]), last[1](last[0] - 2, last[3]), held)
            held = turn(at(1, source), at(0, source), last[1](last[0] - 1, last[3]), held)

        def steady(g, held, at=at, source=source, target=target):
            return turn(at(g, source), at(g - 1, source), at(g - 2, target), held)

        held = lax.fori_loop(2, count, steady, held)
        last = (count, at, source, target)
    tail = turn(None, last[1](last[0] - 1, last[2]), last[1](last[0] - 2, None), held)
    turn(None, None, last[1](last[0] - 1, None), tail)
    for a in range(own_blocks):
        u = even[0][PAD + reach + a, :3]
        out[:, a, :] = u * (1.0 / SCALE) if copies else u
    if copies:
        protein = out[:, 0, :]

        def spread(index, carry):
            shared[index] = protein
            return carry

        lax.fori_loop(0, copies, spread, 0)


def blend_kernel(images, slabs, brackets, codes, own, before, after, proteins, out, fraction):
    here = lax.axis_index("image")
    lower = brackets[0]
    zero = jnp.zeros((1, 1), jnp.float32)
    arcs = [zero]
    for k in range(1, images):
        d = proteins[k * slabs : (k + 1) * slabs] - proteins[(k - 1) * slabs : k * slabs]
        square = jnp.sum(jnp.sum(d * d, axis=0), axis=0, keepdims=True)
        square = jnp.sum(square, axis=1, keepdims=True)
        arcs.append(arcs[-1] + jnp.sqrt(square + EPSILON))
    total = arcs[-1]
    arc_here, arc_lower, arc_upper = zero, zero, zero
    for k in range(images):
        arc_here = jnp.where(here == k, arcs[k], arc_here)
        arc_lower = jnp.where(lower == k, arcs[k], arc_lower)
        arc_upper = jnp.where(lower + 1 == k, arcs[k], arc_upper)
    base = jnp.full((1, 1), lower, jnp.int32).astype(jnp.float32)
    code = jnp.full((1, 1), codes[0], jnp.int32).astype(jnp.float32)
    target = (base + code / CODE_SCALE) / (images - 1)
    weight = (target * total - arc_lower) / (arc_upper - arc_lower)
    mine, previous, following = own[...], before[...], after[...]
    below = jnp.where(lower == here, mine, previous)
    above = jnp.where(lower == here, following, mine)
    weight = jnp.reshape(weight, (1, 1, 1))
    out[...] = (1.0 - weight) * below + weight * above
    fraction[...] = arc_here / total


VMEM = pl.BlockSpec(memory_space=pltpu.VMEM)
SMEM = pl.BlockSpec(memory_space=pltpu.SMEM)


def around(cells, near):
    count = lax.axis_size("space")
    found = []
    for distance in range(-near, near + 1):
        route = [((i + distance) % count, i) for i in range(count)]
        found.append(lax.ppermute(cells, "space", route) if distance else cells)
    return found


def evolve(steps, copies, table, slabs, anchors):
    shape = slabs[0].shape
    near = len(slabs) // 2
    blocks = shape[1] + 2 * HALO * steps + 2 * PAD
    outs = [jax.ShapeDtypeStruct(shape, jnp.float32)]
    if copies:
        outs.append(jax.ShapeDtypeStruct((copies, 3, PROT_DEV), jnp.float32))
    half = [
        pltpu.VMEM((blocks, ROWS, BLOCK), jnp.float32),
        pltpu.VMEM((blocks, BLOCK, WIDTH), jnp.bfloat16),
        pltpu.VMEM((blocks, HALF, BLOCK), jnp.bfloat16),
        pltpu.VMEM((blocks, BLOCK, 3 * BLOCK), jnp.float32),
    ]
    return pl.pallas_call(
        functools.partial(evolve_kernel, steps, near, copies),
        out_shape=outs,
        in_specs=[SMEM] + [VMEM] * (len(slabs) + len(anchors)),
        out_specs=[VMEM] * len(outs),
        scratch_shapes=[
            pltpu.VMEM((blocks, ROWS, BLOCK), jnp.float32),
            pltpu.VMEM((2, WIDTH, 2 * BLOCK), jnp.bfloat16),
            pltpu.SMEM((table.shape[0] * blocks,), jnp.int32),
            pltpu.VMEM((GROUP // 2, table.shape[0], BLOCK, 2 * BLOCK), jnp.float32),
            *half,
            *half,
        ],
        compiler_params=pltpu.CompilerParams(vmem_limit_bytes=32 << 20),
    )(table, *slabs, *anchors)


def body(positions, neighbours, brackets, codes):
    slabs = lax.axis_size("space")
    images = lax.axis_size("image")
    own_blocks = positions.shape[2] // BLOCK
    cells = positions.reshape(3, own_blocks, BLOCK)
    table = neighbours.T
    first = around(cells, -(-HALO * PHASES[0] // own_blocks))
    first[len(first) // 2] = cells * SCALE
    (middle,) = evolve(PHASES[0], 0, table, first, [])
    near = -(-HALO * PHASES[1] // own_blocks)
    skip = len(first) // 2 - near
    anchors = first[skip : len(first) - skip]
    evolved, shared = evolve(PHASES[1], slabs * images, table, around(middle, near), anchors)
    up = [(i, i + 1) for i in range(images - 1)]
    down = [(i + 1, i) for i in range(images - 1)]
    proteins = lax.all_to_all(shared, ("image", "space"), 0, 0, tiled=True)
    before = lax.ppermute(evolved, "image", up)
    after = lax.ppermute(evolved, "image", down)
    new_images, fraction = pl.pallas_call(
        functools.partial(blend_kernel, images, slabs),
        out_shape=(
            jax.ShapeDtypeStruct(cells.shape, jnp.float32),
            jax.ShapeDtypeStruct((1, 1), jnp.float32),
        ),
        in_specs=[SMEM, SMEM, VMEM, VMEM, VMEM, VMEM],
        out_specs=(VMEM, VMEM),
        compiler_params=pltpu.CompilerParams(vmem_limit_bytes=8 << 20),
    )(brackets, codes, evolved, before, after, proteins)
    return new_images.reshape(positions.shape), fraction.reshape(1)


def solution(mesh):
    placed = (P("image", None, "space"), P(), P("image"), P("image"))
    return jax.shard_map(
        body,
        mesh=mesh,
        in_specs=placed,
        out_specs=(P("image", None, "space"), P("image")),
        check_vma=False,
    )
```

```python
import functools
import math

import jax
import jax.numpy as jnp
from jax import lax
from jax.experimental import pallas as pl
from jax.experimental.pallas import tpu as pltpu
from jax.sharding import PartitionSpec as P

PROT_DEV = 128
BLOCK = 128
HALO = 2
STEPS = 10

TIME_STEP = 0.05
RESTRAINT = 1.0
COUPLING = 3.0
KERNEL_RATE = 0.125
EPSILON = 1e-06
CODE_SCALE = 65536.0

SCALE = math.sqrt(2.0 * KERNEL_RATE * math.log2(math.e))
ROWS = 8
SUB = 8
GROUP = 4
LOAD_GROUP = 8
PAD = GROUP
HALF = 8 * ROWS
WIDTH = 2 * HALF
PHASES = (6, 4)


def parts_of(v):
    first = v.astype(jnp.bfloat16).astype(jnp.float32)
    rest = v - first
    second = rest.astype(jnp.bfloat16).astype(jnp.float32)
    return first, second, rest - second


def row_ids():
    return lax.broadcasted_iota(jnp.int32, (ROWS, BLOCK), 0)


def spread_matrices():
    row = lax.broadcasted_iota(jnp.int32, (WIDTH, 2 * BLOCK), 0)
    column = lax.broadcasted_iota(jnp.int32, (WIDTH, 2 * BLOCK), 1) // BLOCK

    def picked(inner, component):
        return (inner == component) | (inner == component + 2 * ROWS) | (inner == component + 5 * ROWS)

    plane = picked(row, column)
    depth = picked(row - HALF * column, 2)
    return [jnp.where(chosen, 1.0, 0.0).astype(jnp.bfloat16) for chosen in (plane, depth)]


def multiply(left, right):
    return lax.dot_general(left, right, (((1,), (0,)), ((), ())), preferred_element_type=jnp.float32)


def side_by_side(low, high):
    lane = lax.broadcasted_iota(jnp.int32, (BLOCK, WIDTH), 1)
    return jnp.where(lane < HALF, low, high)


def place(new, base, refs, picks):
    state, left_feat, right_feat, columns = refs
    rows = row_ids()
    talls = []
    for g, u in enumerate(new):
        u = jnp.where(rows < 3, u, 0.0)
        norm = -0.5 * jnp.sum(u * u, axis=0, keepdims=True)
        left = jnp.where(rows == 3, norm, jnp.where(rows == 4, 1.0, u))
        right = jnp.where(rows == 4, norm, jnp.where(rows == 3, 1.0, u))
        state[base + g] = u
        l1, l2, l3 = parts_of(left)
        r1, r2, r3 = parts_of(right)
        zero = jnp.zeros_like(u)
        stacked = [l1, l1, l2, l2, l1, l3, zero, zero]
        tall = jnp.concatenate(stacked, axis=0).T.astype(jnp.bfloat16)
        left_feat[base + g] = tall
        right_feat[base + g] = jnp.concatenate([r1, r2, r1, r2, r3, r1, zero, zero], axis=0).astype(jnp.bfloat16)
        columns[base + g, :, : 2 * BLOCK] = multiply(tall, picks[0, :HALF])
        columns[base + g, :, 2 * BLOCK :] = jnp.broadcast_to(u.T[:, 2:3], (BLOCK, BLOCK))


def evolve_kernel(
    steps, near, copies, table, *refs,
):
    slabs, refs = refs[: 2 * near + 1], refs[2 * near + 1 :]
    if copies:
        anchors, refs = refs[: 2 * near + 1], refs[2 * near + 1 :]
        out, shared, refs = refs[0], refs[1], refs[2:]
    else:
        anchors, out, refs = slabs, refs[0], refs[1:]
    first, picks, others, weights, even, odd = refs[0], refs[1], refs[2], refs[3], refs[4:8], refs[8:]
    own_blocks = out.shape[1]
    partners = table.shape[0]
    total = table.shape[1]
    reach = HALO * steps
    blocks = own_blocks + 2 * reach
    slab = lax.axis_index("space")
    slabs_around = total // own_blocks
    picks[0], picks[1] = spread_matrices()
    filler = jnp.zeros((ROWS - 3, BLOCK), jnp.float32)

    def scaled(ref, block, ready):
        x = ref[:, block, :]
        return jnp.concatenate([x if ready else x * SCALE, filler], axis=0)

    for index in range(2 * near + 1):
        shift = (index - near) * own_blocks + reach
        begin, end = max(0, -shift), min(own_blocks, blocks - shift)
        size = LOAD_GROUP if (end - begin) % LOAD_GROUP == 0 else GROUP

        def load(turn, carry, index=index, begin=begin, shift=shift, size=size):
            block = begin + turn * size
            for g in range(size):
                spot = block + g + shift + PAD
                first[spot] = scaled(anchors[index], block + g, index == near)
                row = lax.rem((slab + index - near + slabs_around) * own_blocks + block + g, total)
                for k in range(partners):
                    others[spot * partners + k] = spot + table[k, row] - HALO
            new = [scaled(slabs[index], block + g, copies or index == near) for g in range(size)]
            place(new, block + shift + PAD, even, picks)
            return carry

        lax.fori_loop(0, (end - begin) // size, load, 0)
    for spot in [*range(PAD), *range(PAD + blocks, 2 * PAD + blocks)]:
        for k in range(partners):
            others[spot * partners + k] = PAD

    def partners_of(base):
        spot = base * partners
        return tuple(tuple(others[spot + (g * partners + k)] for k in range(partners)) for g in range(GROUP))

    def power(base, source, near_blocks, g, k):
        return multiply(source[1][near_blocks[g][k]], source[2][base + g])

    def gather(sums, source, near_blocks, g, k):
        columns = source[3]
        other = near_blocks[g][k]
        for r in range(0, BLOCK, SUB):
            piece = weights[g, k, r : r + SUB]
            terms = [piece * columns[other, r : r + SUB, c * BLOCK : (c + 1) * BLOCK] for c in range(3)] + [piece]
            sums = terms if sums is None else [total_ + term for total_, term in zip(sums, terms)]
        return sums

    def moved(base, source, sums, g):
        state = source[0]
        rows = row_ids()
        block = base + g
        sx, sy, sz, sw = [jnp.sum(s, axis=0, keepdims=True) for s in sums]
        pulled = jnp.where(rows == 0, sx, jnp.where(rows == 1, sy, sz))
        u = state[block]
        force = (COUPLING / (partners * BLOCK)) * (u * sw - pulled)
        inner = lax.rem(block - (PAD + reach) + own_blocks * near, own_blocks)
        hold = jnp.where(inner * BLOCK < PROT_DEV, RESTRAINT, 0.0)
        return u + TIME_STEP * (force - hold * (u - first[block]))

    def turn(ask, move, store, carried):
        held, near_blocks = carried
        asked = partners_of(ask[0]) if ask else None
        new = () if move else held
        for p in range(GROUP // 2):
            sums = [None, None]
            for k in range(partners):
                found = [power(*ask, asked, 2 * p + g, k) for g in range(2)] if ask else None
                if move:
                    sums = [gather(sums[g], move[1], near_blocks, 2 * p + g, k) for g in range(2)]
                if ask:
                    for g in range(2):
                        weights[2 * p + g, k] = jnp.exp2(found[g])
            if move:
                new += tuple(moved(*move, sums[g], 2 * p + g) for g in range(2))
            if store:
                base, target = store
                if target is None:
                    for g in (2 * p, 2 * p + 1):
                        even[0][base + g] = held[g]
                else:
                    place(held[2 * p : 2 * p + 2], base + 2 * p, target, picks)
        return new, asked

    halves = (even, odd)
    last = None
    for t in range(steps):
        source, target = halves[t % 2], halves[1 - t % 2] if t < steps - 1 else None
        low = HALO * (t + 1) + PAD
        count = (blocks + 2 * PAD - 2 * low) // GROUP

        def at(g, refs, low=low):
            return low + g * GROUP, refs

        if t == 0:
            held = turn(at(0, source), None, None, (None, None))
            held = turn(at(1, source), at(0, source), None, held)
        elif last[0] < 4:
            tail = turn(None, last[1](last[0] - 1, last[2]), last[1](last[0] - 2, last[3]), held)
            held = turn(at(0, source), None, last[1](last[0] - 1, last[3]), tail)
            held = turn(at(1, source), at(0, source), None, held)
        else:
            held = turn(at(0, source), last[1](last[0] - 1, last[2]), last[1](last[0] - 2, last[3]), held)
            held = turn(at(1, source), at(0, source), last[1](last[0] - 1, last[3]), held)

        def steady(g, held, at=at, source=source, target=target):
            return turn(at(g, source), at(g - 1, source), at(g - 2, target), held)

        held = lax.fori_loop(2, count, steady, held)
        last = (count, at, source, target)
    tail = turn(None, last[1](last[0] - 1, last[2]), last[1](last[0] - 2, None), held)
    turn(None, None, last[1](last[0] - 1, None), tail)
    for a in range(own_blocks):
        u = even[0][PAD + reach + a, :3]
        out[:, a, :] = u * (1.0 / SCALE) if copies else u
    if copies:
        protein = out[:, 0, :]

        def spread(index, carry):
            shared[index] = protein
            return carry

        lax.fori_loop(0, copies, spread, 0)


def blend_kernel(images, slabs, brackets, codes, own, before, after, proteins, out, fraction):
    here = lax.axis_index("image")
    lower = brackets[0]
    zero = jnp.zeros((1, 1), jnp.float32)
    arcs = [zero]
    for k in range(1, images):
        d = proteins[k * slabs : (k + 1) * slabs] - proteins[(k - 1) * slabs : k * slabs]
        square = jnp.sum(jnp.sum(d * d, axis=0), axis=0, keepdims=True)
        square = jnp.sum(square, axis=1, keepdims=True)
        arcs.append(arcs[-1] + jnp.sqrt(square + EPSILON))
    total = arcs[-1]
    arc_here, arc_lower, arc_upper = zero, zero, zero
    for k in range(images):
        arc_here = jnp.where(here == k, arcs[k], arc_here)
        arc_lower = jnp.where(lower == k, arcs[k], arc_lower)
        arc_upper = jnp.where(lower + 1 == k, arcs[k], arc_upper)
    base = jnp.full((1, 1), lower, jnp.int32).astype(jnp.float32)
    code = jnp.full((1, 1), codes[0], jnp.int32).astype(jnp.float32)
    target = (base + code / CODE_SCALE) / (images - 1)
    weight = (target * total - arc_lower) / (arc_upper - arc_lower)
    mine, previous, following = own[...], before[...], after[...]
    below = jnp.where(lower == here, mine, previous)
    above = jnp.where(lower == here, following, mine)
    weight = jnp.reshape(weight, (1, 1, 1))
    out[...] = (1.0 - weight) * below + weight * above
    fraction[...] = arc_here / total


VMEM = pl.BlockSpec(memory_space=pltpu.VMEM)
SMEM = pl.BlockSpec(memory_space=pltpu.SMEM)


def around(cells, near):
    count = lax.axis_size("space")
    found = []
    for distance in range(-near, near + 1):
        route = [((i + distance) % count, i) for i in range(count)]
        found.append(lax.ppermute(cells, "space", route) if distance else cells)
    return found


def evolve(steps, copies, table, slabs, anchors):
    shape = slabs[0].shape
    near = len(slabs) // 2
    blocks = shape[1] + 2 * HALO * steps + 2 * PAD
    outs = [jax.ShapeDtypeStruct(shape, jnp.float32)]
    if copies:
        outs.append(jax.ShapeDtypeStruct((copies, 3, PROT_DEV), jnp.float32))
    half = [
        pltpu.VMEM((blocks, ROWS, BLOCK), jnp.float32),
        pltpu.VMEM((blocks, BLOCK, HALF), jnp.bfloat16),
        pltpu.VMEM((blocks, HALF, BLOCK), jnp.bfloat16),
        pltpu.VMEM((blocks, BLOCK, 3 * BLOCK), jnp.float32),
    ]
    return pl.pallas_call(
        functools.partial(evolve_kernel, steps, near, copies),
        out_shape=outs,
        in_specs=[SMEM] + [VMEM] * (len(slabs) + len(anchors)),
        out_specs=[VMEM] * len(outs),
        scratch_shapes=[
            pltpu.VMEM((blocks, ROWS, BLOCK), jnp.float32),
            pltpu.VMEM((2, WIDTH, 2 * BLOCK), jnp.bfloat16),
            pltpu.SMEM((table.shape[0] * blocks,), jnp.int32),
            pltpu.VMEM((GROUP, table.shape[0], BLOCK, BLOCK), jnp.float32),
            *half,
            *half,
        ],
        compiler_params=pltpu.CompilerParams(vmem_limit_bytes=32 << 20),
    )(table, *slabs, *anchors)


def body(positions, neighbours, brackets, codes):
    slabs = lax.axis_size("space")
    images = lax.axis_size("image")
    own_blocks = positions.shape[2] // BLOCK
    cells = positions.reshape(3, own_blocks, BLOCK)
    table = neighbours.T
    first = around(cells, -(-HALO * PHASES[0] // own_blocks))
    first[len(first) // 2] = cells * SCALE
    (middle,) = evolve(PHASES[0], 0, table, first, [])
    near = -(-HALO * PHASES[1] // own_blocks)
    skip = len(first) // 2 - near
    anchors = first[skip : len(first) - skip]
    evolved, shared = evolve(PHASES[1], slabs * images, table, around(middle, near), anchors)
    up = [(i, i + 1) for i in range(images - 1)]
    down = [(i + 1, i) for i in range(images - 1)]
    proteins = lax.all_to_all(shared, ("image", "space"), 0, 0, tiled=True)
    before = lax.ppermute(evolved, "image", up)
    after = lax.ppermute(evolved, "image", down)
    new_images, fraction = pl.pallas_call(
        functools.partial(blend_kernel, images, slabs),
        out_shape=(
            jax.ShapeDtypeStruct(cells.shape, jnp.float32),
            jax.ShapeDtypeStruct((1, 1), jnp.float32),
        ),
        in_specs=[SMEM, SMEM, VMEM, VMEM, VMEM, VMEM],
        out_specs=(VMEM, VMEM),
        compiler_params=pltpu.CompilerParams(vmem_limit_bytes=8 << 20),
    )(brackets, codes, evolved, before, after, proteins)
    return new_images.reshape(positions.shape), fraction.reshape(1)


def solution(mesh):
    placed = (P("image", None, "space"), P(), P("image"), P("image"))
    return jax.shard_map(
        body,
        mesh=mesh,
        in_specs=placed,
        out_specs=(P("image", None, "space"), P("image")),
        check_vma=False,
    )
```

```python
import functools
import math

import jax
import jax.numpy as jnp
from jax import lax
from jax.experimental import pallas as pl
from jax.experimental.pallas import tpu as pltpu
from jax.sharding import PartitionSpec as P

PROT_DEV = 128
BLOCK = 128
HALO = 2
STEPS = 10

TIME_STEP = 0.05
RESTRAINT = 1.0
COUPLING = 3.0
KERNEL_RATE = 0.125
EPSILON = 1e-06
CODE_SCALE = 65536.0

SCALE = math.sqrt(2.0 * KERNEL_RATE * math.log2(math.e))
ROWS = 8
SUB = 8
GROUP = 4
LOAD_GROUP = 8
PAD = GROUP
HALF = 8 * ROWS
WIDTH = 2 * HALF
PHASES = (6, 4)


def parts_of(v):
    first = v.astype(jnp.bfloat16).astype(jnp.float32)
    rest = v - first
    second = rest.astype(jnp.bfloat16).astype(jnp.float32)
    return first, second, rest - second


def row_ids():
    return lax.broadcasted_iota(jnp.int32, (ROWS, BLOCK), 0)


def spread_matrices():
    row = lax.broadcasted_iota(jnp.int32, (WIDTH, 2 * BLOCK), 0)
    column = lax.broadcasted_iota(jnp.int32, (WIDTH, 2 * BLOCK), 1) // BLOCK

    def picked(inner, component):
        return (inner == component) | (inner == component + 2 * ROWS) | (inner == component + 5 * ROWS)

    plane = picked(row, column)
    depth = picked(row - HALF * column, 2)
    return [jnp.where(chosen, 1.0, 0.0).astype(jnp.bfloat16) for chosen in (plane, depth)]


def multiply(left, right):
    return lax.dot_general(left, right, (((1,), (0,)), ((), ())), preferred_element_type=jnp.float32)


def side_by_side(low, high):
    lane = lax.broadcasted_iota(jnp.int32, (BLOCK, WIDTH), 1)
    return jnp.where(lane < HALF, low, high)


def place(new, base, refs, picks):
    state, left_feat, right_feat, columns = refs
    rows = row_ids()
    talls = []
    for g, u in enumerate(new):
        u = jnp.where(rows < 3, u, 0.0)
        norm = -0.5 * jnp.sum(u * u, axis=0, keepdims=True)
        left = jnp.where(rows == 3, norm, jnp.where(rows == 4, 1.0, u))
        right = jnp.where(rows == 4, norm, jnp.where(rows == 3, 1.0, u))
        state[base + g] = u
        l1, l2, l3 = parts_of(left)
        r1, r2, r3 = parts_of(right)
        zero = jnp.zeros_like(u)
        stacked = [l1, l1, l2, l2, l1, l3, zero, zero]
        tall = jnp.concatenate(stacked, axis=0).T.astype(jnp.bfloat16)
        left_feat[base + g] = tall
        right_feat[base + g] = jnp.concatenate([r1, r2, r1, r2, r3, r1, zero, zero], axis=0).astype(jnp.bfloat16)
        columns[base + g, :, : 2 * BLOCK] = multiply(tall, picks[0, :HALF])
        columns[base + g, :, 2 * BLOCK :] = jnp.broadcast_to(u.T[:, 2:3], (BLOCK, BLOCK))


def evolve_kernel(
    steps, near, copies, table, *refs,
):
    slabs, refs = in_order(refs[: 2 * near + 1]), refs[2 * near + 1 :]
    if copies:
        anchors, refs = refs[: 2 * near + 1], refs[2 * near + 1 :]
        out, shared, refs = refs[0], refs[1], refs[2:]
    else:
        anchors, out, refs = slabs, refs[0], refs[1:]
    first, picks, others, weights, even, odd = refs[0], refs[1], refs[2], refs[3], refs[4:8], refs[8:]
    own_blocks = out.shape[1]
    partners = table.shape[0]
    total = table.shape[1]
    reach = HALO * steps
    blocks = own_blocks + 2 * reach
    slab = lax.axis_index("space")
    slabs_around = total // own_blocks
    picks[0], picks[1] = spread_matrices()
    filler = jnp.zeros((ROWS - 3, BLOCK), jnp.float32)

    def scaled(ref, block, ready):
        x = ref[:, block, :]
        return jnp.concatenate([x if ready else x * SCALE, filler], axis=0)

    for index in range(2 * near + 1):
        shift = (index - near) * own_blocks + reach
        begin, end = max(0, -shift), min(own_blocks, blocks - shift)
        size = LOAD_GROUP if (end - begin) % LOAD_GROUP == 0 else GROUP

        def load(turn, carry, index=index, begin=begin, shift=shift, size=size):
            block = begin + turn * size
            for g in range(size):
                spot = block + g + shift + PAD
                first[spot] = scaled(anchors[index], block + g, index == near)
                row = lax.rem((slab + index - near + slabs_around) * own_blocks + block + g, total)
                for k in range(partners):
                    others[spot * partners + k] = spot + table[k, row] - HALO
            new = [scaled(slabs[index], block + g, copies or index == near) for g in range(size)]
            place(new, block + shift + PAD, even, picks)
            return carry

        lax.fori_loop(0, (end - begin) // size, load, 0)
    for spot in [*range(PAD), *range(PAD + blocks, 2 * PAD + blocks)]:
        for k in range(partners):
            others[spot * partners + k] = PAD

    def partners_of(base):
        spot = base * partners
        return tuple(tuple(others[spot + (g * partners + k)] for k in range(partners)) for g in range(GROUP))

    def power(base, source, near_blocks, g, k):
        return multiply(source[1][near_blocks[g][k]], source[2][base + g])

    def gather(sums, source, near_blocks, g, k):
        columns = source[3]
        other = near_blocks[g][k]
        for r in range(0, BLOCK, SUB):
            piece = weights[g, k, r : r + SUB]
            terms = [piece * columns[other, r : r + SUB, c * BLOCK : (c + 1) * BLOCK] for c in range(3)] + [piece]
            sums = terms if sums is None else [total_ + term for total_, term in zip(sums, terms)]
        return sums

    def moved(base, source, sums, g):
        state = source[0]
        rows = row_ids()
        block = base + g
        sx, sy, sz, sw = [jnp.sum(s, axis=0, keepdims=True) for s in sums]
        pulled = jnp.where(rows == 0, sx, jnp.where(rows == 1, sy, sz))
        u = state[block]
        force = (COUPLING / (partners * BLOCK)) * (u * sw - pulled)
        inner = lax.rem(block - (PAD + reach) + own_blocks * near, own_blocks)
        hold = jnp.where(inner * BLOCK < PROT_DEV, RESTRAINT, 0.0)
        return u + TIME_STEP * (force - hold * (u - first[block]))

    def turn(ask, move, store, carried):
        held, near_blocks = carried
        asked = partners_of(ask[0]) if ask else None
        new = () if move else held
        for p in range(GROUP // 2):
            sums = [None, None]
            for k in range(partners):
                found = [power(*ask, asked, 2 * p + g, k) for g in range(2)] if ask else None
                if move:
                    sums = [gather(sums[g], move[1], near_blocks, 2 * p + g, k) for g in range(2)]
                if ask:
                    for g in range(2):
                        weights[2 * p + g, k] = jnp.exp2(found[g])
            if move:
                new += tuple(moved(*move, sums[g], 2 * p + g) for g in range(2))
            if store:
                base, target = store
                if target is None:
                    for g in (2 * p, 2 * p + 1):
                        even[0][base + g] = held[g]
                else:
                    place(held[2 * p : 2 * p + 2], base + 2 * p, target, picks)
        return new, asked

    halves = (even, odd)
    last = None
    for t in range(steps):
        source, target = halves[t % 2], halves[1 - t % 2] if t < steps - 1 else None
        low = HALO * (t + 1) + PAD
        count = (blocks + 2 * PAD - 2 * low) // GROUP

        def at(g, refs, low=low):
            return low + g * GROUP, refs

        if t == 0:
            held = turn(at(0, source), None, None, (None, None))
            held = turn(at(1, source), at(0, source), None, held)
        elif last[0] < 4:
            tail = turn(None, last[1](last[0] - 1, last[2]), last[1](last[0] - 2, last[3]), held)
            held = turn(at(0, source), None, last[1](last[0] - 1, last[3]), tail)
            held = turn(at(1, source), at(0, source), None, held)
        else:
            held = turn(at(0, source), last[1](last[0] - 1, last[2]), last[1](last[0] - 2, last[3]), held)
            held = turn(at(1, source), at(0, source), last[1](last[0] - 1, last[3]), held)

        def steady(g, held, at=at, source=source, target=target):
            return turn(at(g, source), at(g - 1, source), at(g - 2, target), held)

        held = lax.fori_loop(2, count, steady, held)
        last = (count, at, source, target)
    tail = turn(None, last[1](last[0] - 1, last[2]), last[1](last[0] - 2, None), held)
    turn(None, None, last[1](last[0] - 1, None), tail)
    for a in range(own_blocks):
        u = even[0][PAD + reach + a, :3]
        out[:, a, :] = u * (1.0 / SCALE) if copies else u
    if copies:
        protein = out[:, 0, :]

        def spread(index, carry):
            shared[index] = protein
            return carry

        lax.fori_loop(0, copies, spread, 0)


def blend_kernel(images, slabs, brackets, codes, own, before, after, proteins, out, fraction):
    here = lax.axis_index("image")
    lower = brackets[0]
    zero = jnp.zeros((1, 1), jnp.float32)
    arcs = [zero]
    for k in range(1, images):
        d = proteins[k * slabs : (k + 1) * slabs] - proteins[(k - 1) * slabs : k * slabs]
        square = jnp.sum(jnp.sum(d * d, axis=0), axis=0, keepdims=True)
        square = jnp.sum(square, axis=1, keepdims=True)
        arcs.append(arcs[-1] + jnp.sqrt(square + EPSILON))
    total = arcs[-1]
    arc_here, arc_lower, arc_upper = zero, zero, zero
    for k in range(images):
        arc_here = jnp.where(here == k, arcs[k], arc_here)
        arc_lower = jnp.where(lower == k, arcs[k], arc_lower)
        arc_upper = jnp.where(lower + 1 == k, arcs[k], arc_upper)
    base = jnp.full((1, 1), lower, jnp.int32).astype(jnp.float32)
    code = jnp.full((1, 1), codes[0], jnp.int32).astype(jnp.float32)
    target = (base + code / CODE_SCALE) / (images - 1)
    weight = (target * total - arc_lower) / (arc_upper - arc_lower)
    mine, previous, following = own[...], before[...], after[...]
    below = jnp.where(lower == here, mine, previous)
    above = jnp.where(lower == here, following, mine)
    weight = jnp.reshape(weight, (1, 1, 1))
    out[...] = (1.0 - weight) * below + weight * above
    fraction[...] = arc_here / total


VMEM = pl.BlockSpec(memory_space=pltpu.VMEM)
SMEM = pl.BlockSpec(memory_space=pltpu.SMEM)


def around(cells, near):
    count = lax.axis_size("space")
    found = {0: cells}
    for distance in sorted(range(-near, near + 1), key=abs)[1:]:
        route = [((i + distance) % count, i) for i in range(count)]
        found[distance] = lax.ppermute(cells, "space", route)
    return [found[distance] for distance in range(-near, near + 1)]


def nearest_first(count):
    return sorted(range(count), key=lambda index: abs(index - count // 2))


def in_order(slabs):
    return [slabs[nearest_first(len(slabs)).index(index)] for index in range(len(slabs))]


def evolve(steps, copies, table, slabs, anchors):
    shape = slabs[0].shape
    near = len(slabs) // 2
    blocks = shape[1] + 2 * HALO * steps + 2 * PAD
    outs = [jax.ShapeDtypeStruct(shape, jnp.float32)]
    if copies:
        outs.append(jax.ShapeDtypeStruct((copies, 3, PROT_DEV), jnp.float32))
    half = [
        pltpu.VMEM((blocks, ROWS, BLOCK), jnp.float32),
        pltpu.VMEM((blocks, BLOCK, HALF), jnp.bfloat16),
        pltpu.VMEM((blocks, HALF, BLOCK), jnp.bfloat16),
        pltpu.VMEM((blocks, BLOCK, 3 * BLOCK), jnp.float32),
    ]
    return pl.pallas_call(
        functools.partial(evolve_kernel, steps, near, copies),
        out_shape=outs,
        in_specs=[SMEM] + [VMEM] * (len(slabs) + len(anchors)),
        out_specs=[VMEM] * len(outs),
        scratch_shapes=[
            pltpu.VMEM((blocks, ROWS, BLOCK), jnp.float32),
            pltpu.VMEM((2, WIDTH, 2 * BLOCK), jnp.bfloat16),
            pltpu.SMEM((table.shape[0] * blocks,), jnp.int32),
            pltpu.VMEM((GROUP, table.shape[0], BLOCK, BLOCK), jnp.float32),
            *half,
            *half,
        ],
        compiler_params=pltpu.CompilerParams(vmem_limit_bytes=32 << 20),
    )(table, *[slabs[index] for index in nearest_first(len(slabs))], *anchors)


def body(positions, neighbours, brackets, codes):
    slabs = lax.axis_size("space")
    images = lax.axis_size("image")
    own_blocks = positions.shape[2] // BLOCK
    cells = positions.reshape(3, own_blocks, BLOCK)
    table = neighbours.T
    first = around(cells, -(-HALO * PHASES[0] // own_blocks))
    first[len(first) // 2] = cells * SCALE
    (middle,) = evolve(PHASES[0], 0, table, first, [])
    near = -(-HALO * PHASES[1] // own_blocks)
    skip = len(first) // 2 - near
    anchors = first[skip : len(first) - skip]
    evolved, shared = evolve(PHASES[1], slabs * images, table, around(middle, near), anchors)
    up = [(i, i + 1) for i in range(images - 1)]
    down = [(i + 1, i) for i in range(images - 1)]
    proteins = lax.all_to_all(shared, ("image", "space"), 0, 0, tiled=True)
    before = lax.ppermute(evolved, "image", up)
    after = lax.ppermute(evolved, "image", down)
    new_images, fraction = pl.pallas_call(
        functools.partial(blend_kernel, images, slabs),
        out_shape=(
            jax.ShapeDtypeStruct(cells.shape, jnp.float32),
            jax.ShapeDtypeStruct((1, 1), jnp.float32),
        ),
        in_specs=[SMEM, SMEM, VMEM, VMEM, VMEM, VMEM],
        out_specs=(VMEM, VMEM),
        compiler_params=pltpu.CompilerParams(vmem_limit_bytes=8 << 20),
    )(brackets, codes, evolved, before, after, proteins)
    return new_images.reshape(positions.shape), fraction.reshape(1)


def solution(mesh):
    placed = (P("image", None, "space"), P(), P("image"), P("image"))
    return jax.shard_map(
        body,
        mesh=mesh,
        in_specs=placed,
        out_specs=(P("image", None, "space"), P("image")),
        check_vma=False,
    )
```
